256 devices in a mesh: pairs: 2 (over z), band: 128 (over x, y, core).
Axes of the slice: x: 8, y: 8, z: 2, core: 2. Of those that a mesh axis runs over, the one named last changes fastest.
The devices are a block of a 8x8x16 slice.
Arguments:
- query_tiles: bfloat16 [768, 256, 128], P(('pairs', 'band')), parts along dimension 0, may hold values from -52 to 52
- target: bfloat16 [768, 256, 128], P(('pairs', 'band')), parts along dimension 0, may hold values from -6 to 6
- tile_home: int32 [768], P('pairs'), parts along dimension 0, may hold values from 0 to 383, as said below
- candidates: int32 [768, 64], P(('pairs', 'band')), parts along dimension 0, may hold values from 0 to 383, as said below
- valid_mask: int32 [768, 64], P(('pairs', 'band')), parts along dimension 0, may hold values from 0 to 1, as said below
Outputs:
- matched: bfloat16 [768, 256, 128], P(('pairs', 'band')), parts along dimension 0
The draws below stay inside these ranges and needn't reach their ends.
There are 2 independent parts, one for each index of `pairs`. The reference program is written for one: setup_inputs(seed, part) draws one part's arguments, and reference() takes and returns one part's arrays. A program takes and returns all parts, laid end to end along the dimension named above; each array names one. Nothing has to cross between parts.
Inputs may be any that keep to these rules, and one draw needn't show every extreme that they name: `tile_home`: a permutation of 0 to 383; target tile ids that agree modulo 128 are stored on the same device, storage row r lying on device r // 3. Ids in a row are distinct; the candidates of one device's query tiles all lie in one run of 128 consecutive ids taken modulo 384, and its first two query tiles together name every id of that run. `valid_mask`: the first entry of every row is 1.
All inputs are finite; a program needn't handle non-finite values.
Results may differ from the reference program's by a relative error of at most 0.0034.
Values may be sent and summed in bfloat16 or wider, within the bound.
A program may use at most 128 MiB of HBM per device.

```python
import math
import jax
import jax.numpy as jnp
from jax import lax

P_SIZE = 256
C = 128
K = 64
TILES_DEV = 3
NT = 384
WIN = 128
N_BAND = 128


def home_table(key):
    owner_order = jax.random.permutation(jax.random.fold_in(key, 201), N_BAND)
    slot_keys = jax.random.split(jax.random.fold_in(key, 202), N_BAND)
    slot_perms = jax.vmap(lambda subkey: jax.random.permutation(subkey, TILES_DEV))(slot_keys)
    tile_ids = jnp.arange(NT, dtype=jnp.int32)
    residue = tile_ids % N_BAND
    quotient = tile_ids // N_BAND
    return (owner_order[residue] * TILES_DEV + slot_perms[residue, quotient]).astype(jnp.int32)


def candidate_table(key):
    starts = jax.random.randint(jax.random.fold_in(key, 101), (N_BAND,), 0, NT)
    keys_all = jax.random.split(jax.random.fold_in(key, 102), N_BAND * TILES_DEV)
    perms = jax.vmap(lambda subkey: jax.random.permutation(subkey, WIN))(keys_all)
    perms = perms.reshape(N_BAND, TILES_DEV, WIN)
    positions = jnp.concatenate([perms[:, :1, :K], perms[:, :1, K:], perms[:, 2:, :K]], axis=1)
    ident = (starts[:, None, None] + positions) % NT
    return ident.reshape(NT, K).astype(jnp.int32)


def target_table(key):
    base = jnp.clip(jax.random.normal(jax.random.fold_in(key, 301), (NT, P_SIZE, C), jnp.float32), -6.0, 6.0)
    return base


def draw_tile_home(key, part):
    return home_table(key)


def draw_candidates(key, part):
    return candidate_table(key)


def draw_valid_mask(key, part):
    levels = jax.random.randint(jax.random.fold_in(key, 401), (NT, K), 0, 4)
    column = jnp.arange(K, dtype=jnp.int32)[None, :]
    return jnp.where(column == 0, 1, (levels > 0).astype(jnp.int32)).astype(jnp.int32)


def draw_target(key, part):
    return target_table(key).astype(jnp.bfloat16)


def draw_query_tiles(key, part):
    base = jnp.clip(jax.random.normal(jax.random.fold_in(key, 501), (NT, P_SIZE, C), jnp.float32), -6.0, 6.0)
    return base.astype(jnp.bfloat16)


def setup_inputs(seed: int = 0, part: int = 0) -> dict:
    key_of = jax.random.split(jax.random.key(seed), 6)
    own_keys = jax.random.split(jax.random.fold_in(key_of[5], part), 6)
    query_tiles = draw_query_tiles(jax.random.fold_in(jax.random.fold_in(key_of[5], part), 71), part)
    target = draw_target(jax.random.fold_in(jax.random.fold_in(key_of[5], part), 71), part)
    tile_home = draw_tile_home(jax.random.fold_in(jax.random.fold_in(key_of[5], part), 71), part)
    candidates = draw_candidates(jax.random.fold_in(jax.random.fold_in(key_of[5], part), 71), part)
    valid_mask = draw_valid_mask(jax.random.fold_in(jax.random.fold_in(key_of[5], part), 71), part)
    return dict(query_tiles=query_tiles, target=target, tile_home=tile_home, candidates=candidates, valid_mask=valid_mask)


def attend_tile(tile_query, tile_keys, keep_mask):
    per_tile = tile_keys.shape[0] // keep_mask.shape[0]
    scores = jnp.dot(tile_query, tile_keys.T, preferred_element_type=jnp.float32) * (1.0 / math.sqrt(tile_query.shape[1]))
    allowed = jnp.repeat(keep_mask > 0, per_tile)[None, :]
    scores = jnp.where(allowed, scores, -jnp.inf)
    peak = lax.optimization_barrier(jnp.max(scores, axis=1, keepdims=True))
    raised = jnp.exp(scores - peak)
    totals = lax.optimization_barrier(jnp.sum(raised, axis=1, keepdims=True))
    weights = (raised / totals).astype(jnp.bfloat16)
    return jnp.dot(weights, tile_keys, preferred_element_type=jnp.float32).astype(jnp.bfloat16)

def reference(query_tiles, target, tile_home, candidates, valid_mask):

    def one_tile(packed):
        tile_query, chosen, keep_mask = packed
        stored = target[tile_home[chosen]].reshape(-1, target.shape[2])
        return attend_tile(tile_query, stored, keep_mask)
    return lax.map(one_tile, (query_tiles, candidates, valid_mask))
```

```python
import functools
import math

import jax
import jax.numpy as jnp
from jax import lax
from jax.experimental import pallas as pl
from jax.experimental.pallas import tpu as pltpu
from jax.sharding import PartitionSpec as P

NEG = -1e30
MESH = pl.DeviceIdType.MESH
HEAD = (0, -3, 3)
LEAF_B = (-3, 3, 2, -2, 4)
LEAF_A = (0, -1, 1)
LEAF_G = (0, -1, -2, -3, 1, 2, 3, 4)


def ring_slot(way, hop):
    return 3 * way + hop - 1 if hop <= 3 else 6


def row_offset(k):
    return -(k + 1) if k < 3 else (k - 2 if k < 6 else 4)


def kernel(side, bias_ref, sel_ref, q_ref, own_ref, out_ref, *scratch):
    (spine, row, st_a, st_b1u, st_b1d, st_b2u, st_b2d, st_p, kfa, kfb, kfg, tabv, tabs, qt, acc, mx, tot,
     s_spine, r_spine, s_row, r_row, s_a, s_b1u, s_b1d, s_b2u, s_b2d, s_p, r_a, r_b, r_g, s_tab, r_tab, l_tab) = scratch
    n_q, rows_q, channels = q_ref.shape
    half = rows_q // 2
    scale = math.log2(math.e) / math.sqrt(channels)
    me = lax.axis_index("band")
    core = lax.rem(me, 2)
    chip = lax.div(me, 2)
    x, y = lax.div(chip, side), lax.rem(chip, side)
    mine = (1 - core) * x + core * y, (1 - core) * y + core * x

    def place(net, at, dr, ds):
        r, s = lax.rem(at[0] + dr + side, side), lax.rem(at[1] + ds + side, side)
        xx, yy = (1 - net) * r + net * s, (1 - net) * s + net * r
        return (xx * side + yy) * 2

    def dev(dr, ds, other=False):
        return {"band": place(core, mine, dr, ds) + (1 - core if other else core)}

    def source(net, dr, ds):
        if net == 0:
            return place(core, mine, dr, ds) + core
        return place(1 - core, (mine[1], mine[0]), dr, ds) + (1 - core)

    partner = dev(0, 0, True)

    def send(src, dst, ssem, rsem, to):
        pltpu.make_async_remote_copy(
            src_ref=src, dst_ref=dst, send_sem=ssem, recv_sem=rsem, device_id=to, device_id_type=MESH
        ).start()

    def take(ref, sem):
        pltpu.make_async_remote_copy(
            src_ref=ref, dst_ref=ref, send_sem=sem, recv_sem=sem, device_id=partner, device_id_type=MESH
        ).wait_recv()

    def drain(ref, sem):
        pltpu.make_async_remote_copy(
            src_ref=ref, dst_ref=ref, send_sem=sem, recv_sem=sem, device_id=partner, device_id_type=MESH
        ).wait_send()

    barrier = pltpu.get_barrier_semaphore()
    greeted = [partner]
    for d in (-1, 1):
        for other in (False, True):
            greeted += [dev(d, 0, other), dev(0, d, other)]
    for to in greeted:
        pl.semaphore_signal(barrier, inc=1, device_id=to, device_id_type=MESH)
    pl.semaphore_wait(barrier, len(greeted))

    def head(j):
        return own_ref if j == 0 else spine.at[j - 1, 2]

    def spine_send(way, hop, t):
        src = own_ref.at[t] if hop == 1 else spine.at[way, hop - 2, t]
        send(src, spine.at[way, hop - 1, t], s_spine, r_spine.at[way, hop - 1, t], dev(0, 1 - 2 * way))

    def row_send(j, way, hop, t):
        src = head(j).at[t] if hop == 1 else row.at[j, ring_slot(way, hop - 1), t]
        dst = row.at[j, ring_slot(way, hop), t]
        sem = r_row.at[j, ring_slot(way, hop), t]
        if hop == 4:
            part = pl.ds(way * half, half)
            src, dst, sem = src.at[part], dst.at[part], r_row.at[j, 6 + way, t]
        send(src, dst, s_row.at[j], sem, dev(1 - 2 * way, 0))

    def row_take(j, way, hop, t):
        ref = row.at[j, ring_slot(way, hop), t]
        if hop == 4:
            take(ref.at[pl.ds(way * half, half)], r_row.at[j, 6 + way, t])
        else:
            take(ref, r_row.at[j, ring_slot(way, hop), t])

    send(sel_ref, tabv.at[0], s_tab, r_tab, dev(0, -1))
    send(sel_ref, tabv.at[1], s_tab, r_tab, dev(0, 1))
    send(sel_ref, tabv.at[2], s_tab, r_tab, dev(-1, 0, True))
    send(sel_ref, tabv.at[3], s_tab, r_tab, dev(1, 0, True))
    send(sel_ref, tabv.at[4], s_tab, r_tab, partner)
    for t in range(3):
        for way in range(2):
            spine_send(way, 1, t)
            row_send(0, way, 1, t)
    own_tab = pltpu.make_async_copy(sel_ref, tabs.at[5], l_tab.at[0])
    own_tab.start()

    for q in range(n_q):
        qt[:, pl.ds(q * rows_q, rows_q)] = q_ref[q].T
    acc[...] = jnp.zeros_like(acc)
    tot[...] = jnp.zeros_like(tot)
    mx[...] = jnp.full_like(mx, NEG)

    own_tab.wait()
    take(tabv, r_tab)
    got = pltpu.make_async_copy(tabv, tabs.at[pl.ds(0, 5)], l_tab.at[1])
    got.start()
    got.wait()

    def pack(src, who, outs):
        step = 64
        for lo in range(0, rows_q, step):
            tiles = [src[t, pl.ds(lo, step), :] for t in range(3)]
            for table, dst, first, count in outs:
                if first <= lo < first + count:
                    which = tabs[table, 0, who]
                    dst[pl.ds(lo - first, step), :] = jnp.where(
                        which == 0, tiles[0], jnp.where(which == 1, tiles[1], tiles[2])
                    )

    up = (dev(0, 1), dev(0, 1, True))
    down = (dev(0, -1), dev(0, -1, True))
    whole = (0, rows_q)
    low, high = (0, half), (half, half)

    def pack_trunk(src, who, place_self, index_p, place_p, sem_p, more):
        outs = [(5, place_self, *whole), (4, st_p.at[index_p], *whole)]
        outs += [(table, stage, *rng) for table, stage, rng, *_ in more]
        pack(src, who, outs)
        for _, stage, _, dst, ssem, rsem, to in more:
            send(stage, dst, ssem, rsem, to)
        send(st_p.at[index_p], place_p, s_p, sem_p, partner)

    def pack_row(j, k):
        who = source(0, row_offset(k), HEAD[j])
        more = []
        for o in range(2):
            t_up, t_dn = 2 * o, 2 * o + 1
            if j == 0:
                more.append((t_up, st_a.at[k, o], whole, kfa.at[o, k, 1], s_a, r_a.at[o, k], up[o]))
                more.append((t_dn, st_a.at[k, 2 + o], whole, kfa.at[o, k, 2], s_a, r_a.at[o, k], down[o]))
            elif j == 1:
                more.append((t_dn, st_b1d.at[k, o], whole, kfb.at[o, k, 3], s_b1d, r_b.at[o, k], down[o]))
                more.append((t_up, st_b1u.at[k, o], low, kfb.at[o, k, 4, pl.ds(0, half)], s_b1u, r_b.at[o, k], up[o]))
            else:
                more.append((t_up, st_b2u.at[k, o], whole, kfb.at[o, k, 2], s_b2u, r_b.at[o, k], up[o]))
                more.append((t_dn, st_b2d.at[k, o], high, kfb.at[o, k, 4, pl.ds(half, half)], s_b2d, r_b.at[o, k], down[o]))
        if j == 0:
            pack_trunk(row.at[j, k], who, kfa.at[0, k, 0], 7 + k, kfa.at[1, k, 0], r_a.at[1, k], more)
        else:
            pack_trunk(row.at[j, k], who, kfb.at[0, k, j - 1], 7 + 7 * j + k, kfb.at[1, k, j - 1], r_b.at[1, k], more)

    def pack_spine(way, hop):
        slot = 3 * way + hop
        more = []
        if hop == 3:
            for o in range(2):
                if way == 0:
                    more.append((2 * o, st_b1u.at[7, o], low, kfg.at[o, 7, pl.ds(0, half)], s_b1u, r_g.at[o], up[o]))
                else:
                    more.append((2 * o + 1, st_b2d.at[7, o], high, kfg.at[o, 7, pl.ds(half, half)], s_b2d, r_g.at[o], down[o]))
        pack_trunk(spine.at[way, hop - 1], source(0, 0, LEAF_G[slot]), kfg.at[0, slot], slot, kfg.at[1, slot], r_g.at[1], more)

    pack_trunk(own_ref, me, kfg.at[0, 0], 0, kfg.at[1, 0], r_g.at[1], [])

    for hop in range(1, 4):
        for t in range(3):
            for way in range(2):
                take(spine.at[way, hop - 1, t], r_spine.at[way, hop - 1, t])
                if hop < 3:
                    spine_send(way, hop + 1, t)
                else:
                    for w in range(2):
                        row_send(1 + way, w, 1, t)
        for t in range(3):
            for way in range(2):
                row_take(0, way, hop, t)
                row_send(0, way, hop + 1, t)
        for way in range(2):
            pack_row(0, ring_slot(way, hop))
            pack_spine(way, hop)
    for t in range(3):
        for way in range(2):
            row_take(0, way, 4, t)
    pack_row(0, 6)
    for hop in range(1, 5):
        for j in (1, 2):
            for t in range(3):
                for way in range(2):
                    row_take(j, way, hop, t)
                    if hop < 4:
                        row_send(j, way, hop + 1, t)
            for way in range(2 if hop < 4 else 1):
                pack_row(j, ring_slot(way, hop))

    def attend(ref, whos):
        count = len(whos)
        keys = ref[...].reshape(count * rows_q, channels)
        keys_t = keys.T
        for q in range(n_q):
            cols = pl.ds(q * rows_q, rows_q)
            s = jnp.dot(keys, qt[:, cols], preferred_element_type=jnp.float32)
            parts = [s[t * rows_q:(t + 1) * rows_q] for t in range(count)]
            bias = [bias_ref[q, who] for who in whos]
            tops = [jnp.max(p, axis=0, keepdims=True) * scale for p in parts]
            before = mx[q]
            now = before
            for t in range(count):
                now = jnp.maximum(now, tops[t] + bias[t])
            alpha = jnp.exp2(before - now)
            total = alpha * tot[q]
            ps = []
            for t in range(count):
                p = jnp.exp2(parts[t] * scale - jnp.maximum(now - bias[t], tops[t]))
                total = total + jnp.sum(p, axis=0, keepdims=True)
                ps.append(p.astype(jnp.bfloat16))
            mx[q] = now
            tot[q] = total
            pv = jnp.dot(keys_t, jnp.concatenate(ps, axis=0), preferred_element_type=jnp.float32)
            acc[:, cols] = acc[:, cols] * alpha + pv

    def dyn_offset(k):
        return jnp.where(k < 3, -(k + 1), jnp.where(k < 6, k - 2, 4))

    for net in range(2):
        take(kfg.at[0, 7] if net == 0 else kfg.at[1], r_g.at[net])

        def unit_g(h, _):
            offs = [jnp.where(h == 0, LEAF_G[t], LEAF_G[4 + t]) for t in range(4)]
            attend(kfg.at[net, pl.ds(4 * h, 4)], [source(net, 0, o) for o in offs])
            return 0

        lax.fori_loop(0, 2, unit_g, 0)

        def unit_a(k, _):
            take(kfa.at[0, k, pl.ds(1, 2)] if net == 0 else kfa.at[1, k], r_a.at[net, k])
            attend(kfa.at[net, k], [source(net, dyn_offset(k), o) for o in LEAF_A])
            return 0

        lax.fori_loop(0, 7, unit_a, 0)

    for net in range(2):
        def unit_b(k, _):
            take(kfb.at[0, k, pl.ds(2, 3)] if net == 0 else kfb.at[1, k], r_b.at[net, k])
            attend(kfb.at[net, k], [source(net, dyn_offset(k), o) for o in LEAF_B])
            return 0

        lax.fori_loop(0, 7, unit_b, 0)

    for q in range(n_q):
        out_ref[q] = (acc[:, pl.ds(q * rows_q, rows_q)] / tot[q]).T.astype(out_ref.dtype)

    drain(spine, s_spine)
    for j in range(3):
        drain(row.at[j], s_row.at[j])
    drain(st_a, s_a)
    drain(st_b1u, s_b1u)
    drain(st_b1d, s_b1d)
    drain(st_b2u, s_b2u)
    drain(st_b2d, s_b2d)
    drain(st_p, s_p)
    drain(tabv, s_tab)


def body(side, query_tiles, target, tile_home, candidates, valid_mask):
    n_band = 2 * side * side
    tiles_dev, rows_q, channels = target.shape
    half = rows_q // 2
    ids = lax.broadcasted_iota(jnp.int32, (1, 1, tile_home.shape[0]), 2)
    stored = jnp.sum(jnp.where(candidates[:, :, None] == ids, tile_home[None, None, :], 0), axis=2)
    hit = (stored // tiles_dev)[:, :, None] == lax.broadcasted_iota(jnp.int32, (1, 1, n_band), 2)
    sel = jnp.sum(jnp.where(hit[:2], (stored % tiles_dev)[:2, :, None], 0), axis=(0, 1))
    sel = jnp.broadcast_to(sel[None, :], (8, n_band))
    used = jnp.any(hit & (valid_mask > 0)[:, :, None], axis=1)
    bias = jnp.where(used, 0.0, NEG).astype(jnp.float32)

    def tile(*lead):
        return pltpu.VMEM((*lead, rows_q, channels), target.dtype)

    def halves(*lead):
        return pltpu.VMEM((*lead, half, channels), target.dtype)

    dma = pltpu.SemaphoreType.DMA
    n_q = query_tiles.shape[0]
    scratch = [
        tile(2, 3, 3), tile(3, 7, 3), tile(7, 4), halves(8, 2), tile(7, 2), tile(7, 2), halves(8, 2), tile(28),
        tile(2, 7, 3), tile(2, 7, 5), tile(2, 8),
        pltpu.VMEM((5, 8, n_band), jnp.int32), pltpu.SMEM((6, 8, n_band), jnp.int32),
        pltpu.VMEM((channels, n_q * rows_q), target.dtype),
        pltpu.VMEM((channels, n_q * rows_q), jnp.float32),
        pltpu.VMEM((n_q, 1, rows_q), jnp.float32), pltpu.VMEM((n_q, 1, rows_q), jnp.float32),
        dma, dma((2, 3, 3)), dma((3,)), dma((3, 8, 3)), dma, dma, dma, dma, dma, dma,
        dma((2, 7)), dma((2, 7)), dma((2,)), dma, dma, dma((2,)),
    ]
    vmem = pl.BlockSpec(memory_space=pltpu.VMEM)
    return pl.pallas_call(
        functools.partial(kernel, side),
        out_shape=jax.ShapeDtypeStruct(query_tiles.shape, query_tiles.dtype),
        in_specs=[pl.BlockSpec(memory_space=pltpu.SMEM), vmem, vmem, vmem],
        out_specs=vmem,
        scratch_shapes=scratch,
        compiler_params=pltpu.CompilerParams(
            collective_id=0, has_side_effects=True, vmem_limit_bytes=60 * 1024 * 1024
        ),
    )(bias, sel, query_tiles, target)


def solution(mesh):
    side = math.isqrt(mesh.shape["band"] // 2)
    in_specs = (
        P(("pairs", "band"), None, None),
        P(("pairs", "band"), None, None),
        P("pairs"),
        P(("pairs", "band"), None),
        P(("pairs", "band"), None),
    )
    out_specs = P(("pairs", "band"), None, None)
    return jax.shard_map(
        functools.partial(body, side), mesh=mesh, in_specs=in_specs, out_specs=out_specs, check_vma=False
    )
```

```python
import functools
import math

import jax
import jax.numpy as jnp
from jax import lax
from jax.experimental import pallas as pl
from jax.experimental.pallas import tpu as pltpu
from jax.sharding import PartitionSpec as P

NEG = -1e30
MESH = pl.DeviceIdType.MESH
HEAD = (0, -3, 3)
LEAF_B = (-3, 3, 2, -2, 4)
LEAF_A = (0, -1, 1)
LEAF_G = (0, -1, -2, -3, 1, 2, 3, 4)


def ring_slot(way, hop):
    return 3 * way + hop - 1 if hop <= 3 else 6


def row_offset(k):
    return -(k + 1) if k < 3 else (k - 2 if k < 6 else 4)


def kernel(side, bias_ref, sel_ref, q_ref, own_ref, out_ref, *scratch):
    (spine, row, st_a, st_b1u, st_b1d, st_b2u, st_b2d, st_p, kfa, kfb, kfg, tabv, tabs, qt, acc, mx, ktb,
     sc0, sc1, sc2, pr0, pr1, pr2, tp0, tp1, tp2, s_spine, r_spine, s_row, r_row, s_a, s_b1u, s_b1d, s_b2u, s_b2d, s_p, r_a, r_b, r_g, s_tab, r_tab, l_tab) = scratch
    n_q, rows_q, channels = q_ref.shape
    half = rows_q // 2
    scale = math.log2(math.e) / math.sqrt(channels)
    me = lax.axis_index("band")
    core = lax.rem(me, 2)
    chip = lax.div(me, 2)
    x, y = lax.div(chip, side), lax.rem(chip, side)
    mine = (1 - core) * x + core * y, (1 - core) * y + core * x

    def place(net, at, dr, ds):
        r, s = lax.rem(at[0] + dr + side, side), lax.rem(at[1] + ds + side, side)
        xx, yy = (1 - net) * r + net * s, (1 - net) * s + net * r
        return (xx * side + yy) * 2

    def dev(dr, ds, other=False):
        return {"band": place(core, mine, dr, ds) + (1 - core if other else core)}

    def source(net, dr, ds):
        n = core * (1 - net) + (1 - core) * net
        return place(n, ((1 - n) * x + n * y, (1 - n) * y + n * x), dr, ds) + n

    partner = dev(0, 0, True)

    def send(src, dst, ssem, rsem, to):
        pltpu.make_async_remote_copy(
            src_ref=src, dst_ref=dst, send_sem=ssem, recv_sem=rsem, device_id=to, device_id_type=MESH
        ).start()

    def take(ref, sem):
        pltpu.make_async_remote_copy(
            src_ref=ref, dst_ref=ref, send_sem=sem, recv_sem=sem, device_id=partner, device_id_type=MESH
        ).wait_recv()

    def drain(ref, sem):
        pltpu.make_async_remote_copy(
            src_ref=ref, dst_ref=ref, send_sem=sem, recv_sem=sem, device_id=partner, device_id_type=MESH
        ).wait_send()

    barrier = pltpu.get_barrier_semaphore()
    greeted = [partner]
    for d in (-1, 1):
        for other in (False, True):
            greeted += [dev(d, 0, other), dev(0, d, other)]
    for to in greeted:
        pl.semaphore_signal(barrier, inc=1, device_id=to, device_id_type=MESH)
    pl.semaphore_wait(barrier, len(greeted))

    def head(j):
        return own_ref if j == 0 else spine.at[j - 1, 2]

    def spine_send(way, hop, t):
        src = own_ref.at[t] if hop == 1 else spine.at[way, hop - 2, t]
        send(src, spine.at[way, hop - 1, t], s_spine, r_spine.at[way, hop - 1, t], dev(0, 1 - 2 * way))

    def row_send(j, way, hop, t):
        src = head(j).at[t] if hop == 1 else row.at[j, ring_slot(way, hop - 1), t]
        dst = row.at[j, ring_slot(way, hop), t]
        sem = r_row.at[j, ring_slot(way, hop), t]
        if hop == 4:
            part = pl.ds(way * half, half)
            src, dst, sem = src.at[part], dst.at[part], r_row.at[j, 6 + way, t]
        send(src, dst, s_row.at[j], sem, dev(1 - 2 * way, 0))

    def row_take(j, way, hop, t):
        ref = row.at[j, ring_slot(way, hop), t]
        if hop == 4:
            take(ref.at[pl.ds(way * half, half)], r_row.at[j, 6 + way, t])
        else:
            take(ref, r_row.at[j, ring_slot(way, hop), t])

    send(sel_ref, tabv.at[0], s_tab, r_tab, dev(0, -1))
    send(sel_ref, tabv.at[1], s_tab, r_tab, dev(0, 1))
    send(sel_ref, tabv.at[2], s_tab, r_tab, dev(-1, 0, True))
    send(sel_ref, tabv.at[3], s_tab, r_tab, dev(1, 0, True))
    send(sel_ref, tabv.at[4], s_tab, r_tab, partner)
    for t in range(3):
        for way in range(2):
            spine_send(way, 1, t)
            row_send(0, way, 1, t)
    own_tab = pltpu.make_async_copy(sel_ref, tabs.at[5], l_tab.at[0])
    own_tab.start()

    for q in range(n_q):
        scaled = q_ref[q].astype(jnp.float32).T * scale
        hi = scaled.astype(qt.dtype)
        qt[q, pl.ds(0, channels), :] = hi
        qt[q, pl.ds(channels, channels), :] = (scaled - hi.astype(jnp.float32)).astype(qt.dtype)
    acc[...] = jnp.zeros_like(acc)
    mx[...] = jnp.full_like(mx, NEG)
    ktb[pl.ds(channels, 16), :] = jnp.ones((16, ktb.shape[1]), ktb.dtype)

    own_tab.wait()
    take(tabv, r_tab)
    got = pltpu.make_async_copy(tabv, tabs.at[pl.ds(0, 5)], l_tab.at[1])
    got.start()
    got.wait()

    def pack(src, who, outs):
        step = 64
        for lo in range(0, rows_q, step):
            tiles = [src[t, pl.ds(lo, step), :] for t in range(3)]
            for table, dst, first, count in outs:
                if first <= lo < first + count:
                    which = tabs[table, 0, who]
                    dst[pl.ds(lo - first, step), :] = jnp.where(
                        which == 0, tiles[0], jnp.where(which == 1, tiles[1], tiles[2])
                    )

    up = (dev(0, 1), dev(0, 1, True))
    down = (dev(0, -1), dev(0, -1, True))
    whole = (0, rows_q)
    low, high = (0, half), (half, half)

    def pack_trunk(src, who, place_self, index_p, place_p, sem_p, more):
        outs = [(5, place_self, *whole), (4, st_p.at[index_p], *whole)]
        outs += [(table, stage, *rng) for table, stage, rng, *_ in more]
        pack(src, who, outs)
        for _, stage, _, dst, ssem, rsem, to in more:
            send(stage, dst, ssem, rsem, to)
        send(st_p.at[index_p], place_p, s_p, sem_p, partner)

    def pack_row(j, k):
        who = source(0, row_offset(k), HEAD[j])
        more = []
        for o in range(2):
            t_up, t_dn = 2 * o, 2 * o + 1
            if j == 0:
                more.append((t_up, st_a.at[k, o], whole, kfa.at[o, k, 1], s_a, r_a.at[o, k], up[o]))
                more.append((t_dn, st_a.at[k, 2 + o], whole, kfa.at[o, k, 2], s_a, r_a.at[o, k], down[o]))
            elif j == 1:
                more.append((t_dn, st_b1d.at[k, o], whole, kfb.at[o, k, 3], s_b1d, r_b.at[o, k], down[o]))
                more.append((t_up, st_b1u.at[k, o], low, kfb.at[o, k, 4, pl.ds(0, half)], s_b1u, r_b.at[o, k], up[o]))
            else:
                more.append((t_up, st_b2u.at[k, o], whole, kfb.at[o, k, 2], s_b2u, r_b.at[o, k], up[o]))
                more.append((t_dn, st_b2d.at[k, o], high, kfb.at[o, k, 4, pl.ds(half, half)], s_b2d, r_b.at[o, k], down[o]))
        if j == 0:
            pack_trunk(row.at[j, k], who, kfa.at[0, k, 0], 7 + k, kfa.at[1, k, 0], r_a.at[1, k], more)
        else:
            pack_trunk(row.at[j, k], who, kfb.at[0, k, j - 1], 7 + 7 * j + k, kfb.at[1, k, j - 1], r_b.at[1, k], more)

    def pack_spine(way, hop):
        slot = 3 * way + hop
        more = []
        if hop == 3:
            for o in range(2):
                if way == 0:
                    more.append((2 * o, st_b1u.at[7, o], low, kfg.at[o, 7, pl.ds(0, half)], s_b1u, r_g.at[o], up[o]))
                else:
                    more.append((2 * o + 1, st_b2d.at[7, o], high, kfg.at[o, 7, pl.ds(half, half)], s_b2d, r_g.at[o], down[o]))
        pack_trunk(spine.at[way, hop - 1], source(0, 0, LEAF_G[slot]), kfg.at[0, slot], slot, kfg.at[1, slot], r_g.at[1], more)

    pack_trunk(own_ref, me, kfg.at[0, 0], 0, kfg.at[1, 0], r_g.at[1], [])

    scores, probs, tops = (sc0, sc1, sc2), (pr0, pr1, pr2), (tp0, tp1, tp2)

    def attend(units, width, ref_of, whos_of):
        keys = width * rows_q

        def score(q, ref):
            for t in range(width):
                k = ref[t]
                s = jnp.dot(jnp.concatenate([k, k], axis=1), qt[q], preferred_element_type=jnp.float32)
                scores[q][pl.ds(t * rows_q, rows_q), :] = s
                tops[q][t] = jnp.max(s, axis=0, keepdims=True)

        def soften(q, bias):
            before = mx[q]
            now = before
            top = [tops[q][t] for t in range(width)]
            for t in range(width):
                now = jnp.maximum(now, top[t] + bias[t])
            for t in range(width):
                rows = pl.ds(t * rows_q, rows_q)
                shift = jnp.maximum(now - bias[t], top[t])
                probs[q][rows, :] = jnp.exp2(scores[q][rows, :] - shift).astype(jnp.bfloat16)
            mx[q] = now
            return jnp.exp2(before - now)

        def mix(q, alpha):
            pv = jnp.dot(ktb[:, pl.ds(0, keys)], probs[q][pl.ds(0, keys), :], preferred_element_type=jnp.float32)
            acc[q] = acc[q] * alpha + pv

        def unit(u, _):
            ref = ref_of(u)
            following = ref_of(jnp.minimum(u + 1, units - 1))
            whos = whos_of(u)
            ktb[pl.ds(0, channels), pl.ds(0, keys)] = ref[...].reshape(keys, channels).T
            alphas = []
            for q in range(n_q):
                score((q + 1) % n_q, ref if q + 1 < n_q else following)
                alphas.append(soften(q, [bias_ref[q, who] for who in whos]))
                if q > 0:
                    mix(q - 1, alphas[q - 1])
            mix(n_q - 1, alphas[n_q - 1])
            return 0

        score(0, ref_of(0))
        lax.fori_loop(0, units, unit, 0)

    def attend_g():
        take(kfg.at[0, 7], r_g.at[0])
        take(kfg.at[1], r_g.at[1])

        def whos(u):
            offs = [jnp.where(lax.rem(u, 2) == 0, LEAF_G[t], LEAF_G[4 + t]) for t in range(4)]
            return [source(lax.div(u, 2), 0, o) for o in offs]

        attend(4, 4, lambda u: kfg.at[lax.div(u, 2), pl.ds(4 * lax.rem(u, 2), 4)], whos)

    def attend_row(hop, ref, sem, skip, offs):
        ways = 2 if hop < 4 else 1
        for way in range(ways):
            k = ring_slot(way, hop)
            take(ref.at[0, k, pl.ds(skip, ref.shape[2] - skip)], sem.at[0, k])
            take(ref.at[1, k], sem.at[1, k])

        def at(u):
            return lax.div(u, ways), lax.rem(u, ways)

        def unit_ref(u):
            net, way = at(u)
            return ref.at[net, 3 * way + hop - 1 if hop < 4 else 6]

        def whos(u):
            net, way = at(u)
            dr = hop * (2 * way - 1) if hop < 4 else 4
            return [source(net, dr, o) for o in offs]

        attend(2 * ways, len(offs), unit_ref, whos)

    def attend_a(hop):
        attend_row(hop, kfa, r_a, 1, LEAF_A)

    def attend_b(hop):
        attend_row(hop, kfb, r_b, 2, LEAF_B)

    for hop in range(1, 4):
        for t in range(3):
            for way in range(2):
                take(spine.at[way, hop - 1, t], r_spine.at[way, hop - 1, t])
                if hop < 3:
                    spine_send(way, hop + 1, t)
                else:
                    for w in range(2):
                        row_send(1 + way, w, 1, t)
        for t in range(3):
            for way in range(2):
                row_take(0, way, hop, t)
                row_send(0, way, hop + 1, t)
        for way in range(2):
            pack_row(0, ring_slot(way, hop))
            pack_spine(way, hop)
    for t in range(3):
        for way in range(2):
            row_take(0, way, 4, t)
    pack_row(0, 6)
    covers = {
        (1, 1): [attend_g], (1, 2): [lambda: attend_a(1)],
        (2, 1): [lambda: attend_a(2)], (2, 2): [lambda: attend_a(3)],
        (3, 1): [lambda: attend_a(4)], (3, 2): [lambda: attend_b(1)],
        (4, 1): [], (4, 2): [lambda: attend_b(2), lambda: attend_b(3), lambda: attend_b(4)],
    }
    for hop in range(1, 5):
        for j in (1, 2):
            for t in range(3):
                for way in range(2):
                    row_take(j, way, hop, t)
                    if hop < 4:
                        row_send(j, way, hop + 1, t)
            for way in range(2 if hop < 4 else 1):
                pack_row(j, ring_slot(way, hop))
            for cover in covers[hop, j]:
                cover()

    for q in range(n_q):
        out_ref[q] = (acc[q, pl.ds(0, channels), :] / acc[q, pl.ds(channels, 1), :]).T.astype(out_ref.dtype)

    drain(spine, s_spine)
    for j in range(3):
        drain(row.at[j], s_row.at[j])
    drain(st_a, s_a)
    drain(st_b1u, s_b1u)
    drain(st_b1d, s_b1d)
    drain(st_b2u, s_b2u)
    drain(st_b2d, s_b2d)
    drain(st_p, s_p)
    drain(tabv, s_tab)


def body(side, query_tiles, target, tile_home, candidates, valid_mask):
    n_band = 2 * side * side
    tiles_dev, rows_q, channels = target.shape
    half = rows_q // 2
    ids = lax.broadcasted_iota(jnp.int32, (1, 1, tile_home.shape[0]), 2)
    stored = jnp.sum(jnp.where(candidates[:, :, None] == ids, tile_home[None, None, :], 0), axis=2)
    hit = (stored // tiles_dev)[:, :, None] == lax.broadcasted_iota(jnp.int32, (1, 1, n_band), 2)
    sel = jnp.sum(jnp.where(hit[:2], (stored % tiles_dev)[:2, :, None], 0), axis=(0, 1))
    sel = jnp.broadcast_to(sel[None, :], (8, n_band))
    used = jnp.any(hit & (valid_mask > 0)[:, :, None], axis=1)
    bias = jnp.where(used, 0.0, NEG).astype(jnp.float32)

    def tile(*lead):
        return pltpu.VMEM((*lead, rows_q, channels), target.dtype)

    def halves(*lead):
        return pltpu.VMEM((*lead, half, channels), target.dtype)

    dma = pltpu.SemaphoreType.DMA
    n_q, widest = query_tiles.shape[0], len(LEAF_B)
    scratch = [
        tile(2, 3, 3), tile(3, 7, 3), tile(7, 4), halves(8, 2), tile(7, 2), tile(7, 2), halves(8, 2), tile(28),
        tile(2, 7, 3), tile(2, 7, 5), tile(2, 8),
        pltpu.VMEM((5, 8, n_band), jnp.int32), pltpu.SMEM((6, 8, n_band), jnp.int32),
        pltpu.VMEM((n_q, 2 * channels, rows_q), target.dtype),
        pltpu.VMEM((n_q, channels + 16, rows_q), jnp.float32),
        pltpu.VMEM((n_q, 1, rows_q), jnp.float32),
        pltpu.VMEM((channels + 16, widest * rows_q), target.dtype),
        *[pltpu.VMEM((widest * rows_q, rows_q), jnp.float32)] * 3,
        *[pltpu.VMEM((widest * rows_q, rows_q), target.dtype)] * 3,
        *[pltpu.VMEM((widest, 1, rows_q), jnp.float32)] * 3,
        dma, dma((2, 3, 3)), dma((3,)), dma((3, 8, 3)), dma, dma, dma, dma, dma, dma,
        dma((2, 7)), dma((2, 7)), dma((2,)), dma, dma, dma((2,)),
    ]
    vmem = pl.BlockSpec(memory_space=pltpu.VMEM)
    return pl.pallas_call(
        functools.partial(kernel, side),
        out_shape=jax.ShapeDtypeStruct(query_tiles.shape, query_tiles.dtype),
        in_specs=[pl.BlockSpec(memory_space=pltpu.SMEM), vmem, vmem, vmem],
        out_specs=vmem,
        scratch_shapes=scratch,
        compiler_params=pltpu.CompilerParams(
            collective_id=0, has_side_effects=True, vmem_limit_bytes=60 * 1024 * 1024
        ),
    )(bias, sel, query_tiles, target)


def solution(mesh):
    side = math.isqrt(mesh.shape["band"] // 2)
    in_specs = (
        P(("pairs", "band"), None, None),
        P(("pairs", "band"), None, None),
        P("pairs"),
        P(("pairs", "band"), None),
        P(("pairs", "band"), None),
    )
    out_specs = P(("pairs", "band"), None, None)
    return jax.shard_map(
        functools.partial(body, side), mesh=mesh, in_specs=in_specs, out_specs=out_specs, check_vma=False
    )
```

```python
import functools
import math

import jax
import jax.numpy as jnp
from jax import lax
from jax.experimental import pallas as pl
from jax.experimental.pallas import tpu as pltpu
from jax.sharding import PartitionSpec as P

NEG = -1e30
MESH = pl.DeviceIdType.MESH
HEAD = (0, -3, 3)
LEAF_B = (-3, 3, 2, -2, 4)
LEAF_A = (0, -1, 1)
LEAF_G = (0, -1, 1, -2, 2, -3, 3, 4)
NEAR = 5
COVERS = {
    (0, 3): ("near",), (1, 1): ("a1",), (2, 1): ("far",), (1, 2): ("a2",), (2, 2): ("a3",),
    (1, 3): ("a4", "b1"), (2, 3): ("b2",), (2, 4): ("b3", "b4"),
}


def ring_slot(way, hop):
    return 3 * way + hop - 1 if hop <= 3 else 6


def row_offset(k):
    return -(k + 1) if k < 3 else (k - 2 if k < 6 else 4)


def kernel(side, home_ref, cand_ref, valid_ref, q_any, own_any, out_ref, *scratch):
    (q_ref, own_ref, spine, row, st_a, st_b1u, st_b1d, st_b2u, st_b2d, st_p, kfa, kfb, kfg, table, tabv, tabs, qt, acc,
     mx, ktb, sc0, sc1, pr0, pr1, tp0, tp1, s_spine, r_spine, s_row, r_row, s_a, s_b1u, s_b1d, s_b2u, s_b2d, s_p,
     r_a, r_b, r_g, s_tab, r_tab, l_tab) = scratch
    load_own = pltpu.make_async_copy(own_any, own_ref, l_tab.at[2])
    load_q = pltpu.make_async_copy(q_any, q_ref, l_tab.at[3])
    load_own.start()
    load_q.start()
    n_q, rows_q, channels = q_ref.shape
    half = rows_q // 2
    scale = math.log2(math.e) / math.sqrt(channels)
    me = lax.axis_index("band")
    core = lax.rem(me, 2)
    chip = lax.div(me, 2)
    x, y = lax.div(chip, side), lax.rem(chip, side)
    mine = (1 - core) * x + core * y, (1 - core) * y + core * x

    def place(net, at, dr, ds):
        r, s = lax.rem(at[0] + dr + side, side), lax.rem(at[1] + ds + side, side)
        xx, yy = (1 - net) * r + net * s, (1 - net) * s + net * r
        return (xx * side + yy) * 2

    def dev(dr, ds, other=False):
        return {"band": place(core, mine, dr, ds) + (1 - core if other else core)}

    def source(net, dr, ds):
        n = core * (1 - net) + (1 - core) * net
        return place(n, ((1 - n) * x + n * y, (1 - n) * y + n * x), dr, ds) + n

    partner = dev(0, 0, True)

    def send(src, dst, ssem, rsem, to):
        pltpu.make_async_remote_copy(
            src_ref=src, dst_ref=dst, send_sem=ssem, recv_sem=rsem, device_id=to, device_id_type=MESH
        ).start()

    def take(ref, sem):
        pltpu.make_async_remote_copy(
            src_ref=ref, dst_ref=ref, send_sem=sem, recv_sem=sem, device_id=partner, device_id_type=MESH
        ).wait_recv()

    def drain(ref, sem):
        pltpu.make_async_remote_copy(
            src_ref=ref, dst_ref=ref, send_sem=sem, recv_sem=sem, device_id=partner, device_id_type=MESH
        ).wait_send()

    barrier = pltpu.get_barrier_semaphore()
    greeted = [partner]
    for d in (-1, 1):
        for other in (False, True):
            greeted += [dev(d, 0, other), dev(0, d, other)]
    for to in greeted:
        pl.semaphore_signal(barrier, inc=1, device_id=to, device_id_type=MESH)
    pl.semaphore_wait(barrier, len(greeted))

    def head(j):
        return own_ref if j == 0 else spine.at[j - 1, 2]

    def spine_send(way, hop, t):
        src = own_ref.at[t] if hop == 1 else spine.at[way, hop - 2, t]
        send(src, spine.at[way, hop - 1, t], s_spine, r_spine.at[way, hop - 1, t], dev(0, 1 - 2 * way))

    def row_send(j, way, hop, t):
        src = head(j).at[t] if hop == 1 else row.at[j, ring_slot(way, hop - 1), t]
        dst = row.at[j, ring_slot(way, hop), t]
        sem = r_row.at[j, ring_slot(way, hop), t]
        if hop == 4:
            part = pl.ds(way * half, half)
            src, dst, sem = src.at[part], dst.at[part], r_row.at[j, 6 + way, t]
        send(src, dst, s_row.at[j], sem, dev(1 - 2 * way, 0))

    def row_take(j, way, hop, t):
        ref = row.at[j, ring_slot(way, hop), t]
        if hop == 4:
            take(ref.at[pl.ds(way * half, half)], r_row.at[j, 6 + way, t])
        else:
            take(ref, r_row.at[j, ring_slot(way, hop), t])

    load_own.wait()
    for t in range(3):
        for way in range(2):
            spine_send(way, 1, t)
            row_send(0, way, 1, t)

    n_band = table.shape[1]
    lane = lax.broadcasted_iota(jnp.int32, (1, n_band), 1)

    def fold(k, rows):
        rows = list(rows)
        for q in range(n_q):
            stored = home_ref[cand_ref[q, k]]
            who = lax.div(stored, own_ref.shape[0])
            hit = lane == who
            if q < 2:
                rows[0] = jnp.where(hit, stored - who * own_ref.shape[0], rows[0])
                rows[4] = jnp.where(hit, q, rows[4])
            rows[1 + q] = jnp.where(hit, valid_ref[q, k], rows[1 + q])
        return tuple(rows)

    blank = jnp.zeros((1, n_band), jnp.int32)
    built = lax.fori_loop(0, cand_ref.shape[1], fold, (blank,) * 5, unroll=8)
    for r in range(5):
        table[pl.ds(r, 1), :] = built[r]
    load_q.wait()
    for q in range(n_q):
        scaled = q_ref[q].astype(jnp.float32).T * scale
        hi = scaled.astype(qt.dtype)
        qt[q, pl.ds(0, channels), :] = hi
        qt[q, pl.ds(channels, channels), :] = (scaled - hi.astype(jnp.float32)).astype(qt.dtype)
    acc[...] = jnp.zeros_like(acc)
    mx[...] = jnp.full_like(mx, NEG)

    send(table, tabv.at[0], s_tab, r_tab, dev(0, -1))
    send(table, tabv.at[1], s_tab, r_tab, dev(0, 1))
    send(table, tabv.at[2], s_tab, r_tab, dev(-1, 0, True))
    send(table, tabv.at[3], s_tab, r_tab, dev(1, 0, True))
    send(table, tabv.at[4], s_tab, r_tab, partner)
    own_tab = pltpu.make_async_copy(table, tabs.at[5], l_tab.at[0])
    own_tab.start()
    own_tab.wait()
    take(tabv, r_tab)
    got = pltpu.make_async_copy(tabv, tabs.at[pl.ds(0, 5)], l_tab.at[1])
    got.start()
    got.wait()

    def pack(src, who, outs):
        step = 64
        for lo in range(0, rows_q, step):
            tiles = [src[t, pl.ds(lo, step), :] for t in range(3)]
            for table, dst, first, count in outs:
                if first <= lo < first + count:
                    which = tabs[table, 0, who]
                    dst[pl.ds(lo - first, step), :] = jnp.where(
                        which == 0, tiles[0], jnp.where(which == 1, tiles[1], tiles[2])
                    )

    up = (dev(0, 1), dev(0, 1, True))
    down = (dev(0, -1), dev(0, -1, True))
    whole = (0, rows_q)
    low, high = (0, half), (half, half)

    def pack_trunk(src, who, place_self, index_p, place_p, sem_p, more):
        outs = [(5, place_self, *whole), (4, st_p.at[index_p], *whole)]
        outs += [(table, stage, *rng) for table, stage, rng, *_ in more]
        pack(src, who, outs)
        for _, stage, _, dst, ssem, rsem, to in more:
            send(stage, dst, ssem, rsem, to)
        send(st_p.at[index_p], place_p, s_p, sem_p, partner)

    def pack_row(j, k):
        who = source(0, row_offset(k), HEAD[j])
        more = []
        for o in range(2):
            t_up, t_dn = 2 * o, 2 * o + 1
            if j == 0:
                more.append((t_up, st_a.at[k, o], whole, kfa.at[o, k, 1], s_a, r_a.at[o, k], up[o]))
                more.append((t_dn, st_a.at[k, 2 + o], whole, kfa.at[o, k, 2], s_a, r_a.at[o, k], down[o]))
            elif j == 1:
                more.append((t_dn, st_b1d.at[k, o], whole, kfb.at[o, k, 3], s_b1d, r_b.at[o, k], down[o]))
                more.append((t_up, st_b1u.at[k, o], low, kfb.at[o, k, 4, pl.ds(0, half)], s_b1u, r_b.at[o, k], up[o]))
            else:
                more.append((t_up, st_b2u.at[k, o], whole, kfb.at[o, k, 2], s_b2u, r_b.at[o, k], up[o]))
                more.append((t_dn, st_b2d.at[k, o], high, kfb.at[o, k, 4, pl.ds(half, half)], s_b2d, r_b.at[o, k], down[o]))
        if j == 0:
            pack_trunk(row.at[j, k], who, kfa.at[0, k, 0], 7 + k, kfa.at[1, k, 0], r_a.at[1, k], more)
        else:
            pack_trunk(row.at[j, k], who, kfb.at[0, k, j - 1], 7 + 7 * j + k, kfb.at[1, k, j - 1], r_b.at[1, k], more)

    def pack_spine(way, hop):
        slot = 2 * hop - 1 + way
        more = []
        if hop == 3:
            for o in range(2):
                if way == 0:
                    more.append((2 * o, st_b1u.at[7, o], low, kfg.at[o, 7, pl.ds(0, half)], s_b1u, r_g.at[2 * o], up[o]))
                else:
                    more.append((2 * o + 1, st_b2d.at[7, o], high, kfg.at[o, 7, pl.ds(half, half)], s_b2d, r_g.at[2 * o], down[o]))
        pack_trunk(spine.at[way, hop - 1], source(0, 0, LEAF_G[slot]), kfg.at[0, slot], slot, kfg.at[1, slot], r_g.at[1 if slot < NEAR else 2], more)

    pack_trunk(own_ref, me, kfg.at[0, 0], 0, kfg.at[1, 0], r_g.at[1], [])

    scores, probs, tops = (sc0, sc1), (pr0, pr1), (tp0, tp1)
    ext = channels + 16

    def attend(units, width, ref_of, whos_of):
        keys = width * rows_q

        def score(v, ref, whos):
            for t in range(width):
                k = ref[t]
                rhs = qt[2] if v == 1 else qt[tabs[5, 4, whos[t]]]
                s = jnp.dot(jnp.concatenate([k, k], axis=1), rhs, preferred_element_type=jnp.float32)
                scores[v][pl.ds(t * rows_q, rows_q), :] = s
                tops[v][t] = jnp.max(s, axis=0, keepdims=True)

        def soften(v, t, shift):
            rows = pl.ds(t * rows_q, rows_q)
            probs[v][rows, :] = jnp.exp2(scores[v][rows, :] - shift).astype(jnp.bfloat16)

        def bias(q, who):
            return jnp.where(tabs[5, 1 + q, who] > 0, 0.0, NEG).astype(jnp.float32)

        def unit(u, _):
            ref, whos = ref_of(u), whos_of(u)
            later = jnp.minimum(u + 1, units - 1)
            second = [tabs[5, 4, who] == 1 for who in whos]
            b = [[bias(q, who) for who in whos] for q in range(3)]
            for t in range(width):
                kt = jnp.concatenate([ref[t].T, jnp.ones((16, rows_q), jnp.bfloat16)], axis=0)
                none = jnp.zeros_like(kt)
                cols = pl.ds(t * rows_q, rows_q)
                ktb[pl.ds(0, ext), cols] = jnp.where(second[t], none, kt)
                ktb[pl.ds(ext, ext), cols] = jnp.where(second[t], kt, none)
                ktb[pl.ds(2 * ext, ext), cols] = kt
            score(1, ref, whos)
            before = [mx[q] for q in range(3)]
            now = list(before)
            for t in range(width):
                for q in range(2):
                    now[q] = jnp.maximum(now[q], tops[0][t] + b[q][t])
            for t in range(width):
                base = jnp.where(second[t], now[1], now[0]) - jnp.maximum(b[0][t], b[1][t])
                soften(0, t, jnp.maximum(base, tops[0][t]))
            pv = jnp.dot(ktb[pl.ds(0, 2 * ext), pl.ds(0, keys)], probs[0][pl.ds(0, keys), :],
                         preferred_element_type=jnp.float32)
            for q in range(2):
                acc[q] = acc[q] * jnp.exp2(before[q] - now[q]) + pv[q * ext:(q + 1) * ext]
            score(0, ref_of(later), whos_of(later))
            for t in range(width):
                now[2] = jnp.maximum(now[2], tops[1][t] + b[2][t])
            for t in range(width):
                soften(1, t, jnp.maximum(now[2] - b[2][t], tops[1][t]))
            pv = jnp.dot(ktb[pl.ds(2 * ext, ext), pl.ds(0, keys)], probs[1][pl.ds(0, keys), :],
                         preferred_element_type=jnp.float32)
            acc[2] = acc[2] * jnp.exp2(before[2] - now[2]) + pv
            for q in range(3):
                mx[q] = now[q]
            return 0

        score(0, ref_of(0), whos_of(0))
        lax.fori_loop(0, units, unit, 0)

    def attend_near():
        take(kfg.at[1, pl.ds(0, NEAR)], r_g.at[1])
        attend(2, NEAR, lambda u: kfg.at[u, pl.ds(0, NEAR)], lambda u: [source(u, 0, o) for o in LEAF_G[:NEAR]])

    def attend_far():
        far = len(LEAF_G) - NEAR
        take(kfg.at[0, 7], r_g.at[0])
        take(kfg.at[1, pl.ds(NEAR, far)], r_g.at[2])
        attend(2, far, lambda u: kfg.at[u, pl.ds(NEAR, far)], lambda u: [source(u, 0, o) for o in LEAF_G[NEAR:]])

    def attend_row(hop, ref, sem, skip, offs):
        ways = 2 if hop < 4 else 1
        for way in range(ways):
            k = ring_slot(way, hop)
            take(ref.at[0, k, pl.ds(skip, ref.shape[2] - skip)], sem.at[0, k])
            take(ref.at[1, k], sem.at[1, k])

        def at(u):
            return lax.div(u, ways), lax.rem(u, ways)

        def unit_ref(u):
            net, way = at(u)
            return ref.at[net, 3 * way + hop - 1 if hop < 4 else 6]

        def whos(u):
            net, way = at(u)
            dr = hop * (2 * way - 1) if hop < 4 else 4
            return [source(net, dr, o) for o in offs]

        attend(2 * ways, len(offs), unit_ref, whos)

    def cover(name):
        if name == "near":
            attend_near()
        elif name == "far":
            attend_far()
        elif name[0] == "a":
            attend_row(int(name[1]), kfa, r_a, 1, LEAF_A)
        else:
            attend_row(int(name[1]), kfb, r_b, 2, LEAF_B)

    def covers(step):
        for name in COVERS.get(step, ()):
            cover(name)

    for hop in range(1, 4):
        for t in range(3):
            for way in range(2):
                take(spine.at[way, hop - 1, t], r_spine.at[way, hop - 1, t])
                if hop < 3:
                    spine_send(way, hop + 1, t)
                else:
                    for w in range(2):
                        row_send(1 + way, w, 1, t)
        for t in range(3):
            for way in range(2):
                row_take(0, way, hop, t)
                row_send(0, way, hop + 1, t)
        for way in range(2):
            pack_row(0, ring_slot(way, hop))
            pack_spine(way, hop)
        covers((0, hop))
    for t in range(3):
        for way in range(2):
            row_take(0, way, 4, t)
    pack_row(0, 6)
    covers((0, 4))
    for hop in range(1, 5):
        for j in (1, 2):
            for t in range(3):
                for way in range(2):
                    row_take(j, way, hop, t)
                    if hop < 4:
                        row_send(j, way, hop + 1, t)
            for way in range(2 if hop < 4 else 1):
                pack_row(j, ring_slot(way, hop))
            covers((j, hop))

    for q in range(n_q):
        out_ref[q] = (acc[q, pl.ds(0, channels), :] / acc[q, pl.ds(channels, 1), :]).T.astype(out_ref.dtype)

    drain(spine, s_spine)
    for j in range(3):
        drain(row.at[j], s_row.at[j])
    drain(st_a, s_a)
    drain(st_b1u, s_b1u)
    drain(st_b1d, s_b1d)
    drain(st_b2u, s_b2u)
    drain(st_b2d, s_b2d)
    drain(st_p, s_p)
    drain(tabv, s_tab)


def body(side, query_tiles, target, tile_home, candidates, valid_mask):
    n_band = 2 * side * side
    tiles_dev, rows_q, channels = target.shape
    half = rows_q // 2

    def tile(*lead):
        return pltpu.VMEM((*lead, rows_q, channels), target.dtype)

    def halves(*lead):
        return pltpu.VMEM((*lead, half, channels), target.dtype)

    dma = pltpu.SemaphoreType.DMA
    n_q, widest = query_tiles.shape[0], len(LEAF_B)
    scratch = [
        tile(n_q), tile(tiles_dev), tile(2, 3, 3), tile(3, 7, 3), tile(7, 4), halves(8, 2), tile(7, 2), tile(7, 2), halves(8, 2), tile(28),
        tile(2, 7, 3), tile(2, 7, 5), tile(2, 8),
        pltpu.VMEM((8, n_band), jnp.int32), pltpu.VMEM((5, 8, n_band), jnp.int32), pltpu.SMEM((6, 8, n_band), jnp.int32),
        pltpu.VMEM((n_q, 2 * channels, rows_q), target.dtype),
        pltpu.VMEM((n_q, channels + 16, rows_q), jnp.float32),
        pltpu.VMEM((n_q, 1, rows_q), jnp.float32),
        pltpu.VMEM((3 * (channels + 16), widest * rows_q), target.dtype),
        *[pltpu.VMEM((widest * rows_q, rows_q), jnp.float32)] * 2,
        *[pltpu.VMEM((widest * rows_q, rows_q), target.dtype)] * 2,
        *[pltpu.VMEM((widest, 1, rows_q), jnp.float32)] * 2,
        dma, dma((2, 3, 3)), dma((3,)), dma((3, 8, 3)), dma, dma, dma, dma, dma, dma,
        dma((2, 7)), dma((2, 7)), dma((3,)), dma, dma, dma((4,)),
    ]
    smem = pl.BlockSpec(memory_space=pltpu.SMEM)
    anywhere = pl.BlockSpec(memory_space=pl.ANY)
    return pl.pallas_call(
        functools.partial(kernel, side),
        out_shape=jax.ShapeDtypeStruct(query_tiles.shape, query_tiles.dtype),
        in_specs=[smem, smem, smem, anywhere, anywhere],
        out_specs=pl.BlockSpec(memory_space=pltpu.VMEM),
        scratch_shapes=scratch,
        compiler_params=pltpu.CompilerParams(
            collective_id=0, has_side_effects=True, vmem_limit_bytes=60 * 1024 * 1024
        ),
    )(tile_home, candidates, valid_mask, query_tiles, target)


def solution(mesh):
    side = math.isqrt(mesh.shape["band"] // 2)
    in_specs = (
        P(("pairs", "band"), None, None),
        P(("pairs", "band"), None, None),
        P("pairs"),
        P(("pairs", "band"), None),
        P(("pairs", "band"), None),
    )
    out_specs = P(("pairs", "band"), None, None)
    return jax.shard_map(
        functools.partial(body, side), mesh=mesh, in_specs=in_specs, out_specs=out_specs, check_vma=False
    )
```

```python
import functools
import math

import jax
import jax.numpy as jnp
from jax import lax
from jax.experimental import pallas as pl
from jax.experimental.pallas import tpu as pltpu
from jax.sharding import PartitionSpec as P

NEG = -1e30
MESH = pl.DeviceIdType.MESH
HEAD = (0, -3, 3)
LEAF_B = (-3, 3, 2, -2, 4)
LEAF_A = (0, -1, 1)
LEAF_G = (0, -1, 1, -2, 2, -3, 3, 4)
NEAR = 5
PLAN = (
    "s1", "init", "r01", "s2", "own", "z1", "s3", "z3", "r02", "z2", "r21", "r11", "p01", "r03", "p21",
    "near", "r22", "p11", "p22", "far", "r12", "p12", "p03", "a1", "p02", "b1", "r04", "r23", "p04", "p23",
    "r13", "p13", "b2", "a3", "r24", "r14", "a2", "p24", "p14", "a4", "b3", "b4",
)


def ring_slot(way, hop):
    return 3 * way + hop - 1 if hop <= 3 else 6


def row_offset(k):
    return -(k + 1) if k < 3 else (k - 2 if k < 6 else 4)


def kernel(side, home_any, cand_any, valid_any, q_any, own_any, out_ref, *scratch):
    (home_ref, cand_ref, valid_ref, q_ref, own_ref, spine, row, st_a, st_b1u, st_b1d, st_b2u, st_b2d, st_p, kfa, kfb, kfg, table, tabv, tabs, qt, acc,
     mx, ktb, sc0, sc1, pr0, pr1, tp0, tp1, s_spine, r_spine, s_row, r_row, s_a, s_b1u, s_b1d, s_b2u, s_b2d, s_p,
     r_a, r_b, r_g, s_tab, r_tab, l_tab) = scratch
    load_own = pltpu.make_async_copy(own_any, own_ref, l_tab.at[2])
    load_q = pltpu.make_async_copy(q_any, q_ref, l_tab.at[3])
    load_tables = [
        pltpu.make_async_copy(src, dst, l_tab.at[4 + i])
        for i, (src, dst) in enumerate(((home_any, home_ref), (cand_any, cand_ref), (valid_any, valid_ref)))
    ]
    for load in (*load_tables, load_own, load_q):
        load.start()
    n_q, rows_q, channels = q_ref.shape
    half = rows_q // 2
    scale = math.log2(math.e) / math.sqrt(channels)
    me = lax.axis_index("band")
    core = lax.rem(me, 2)
    chip = lax.div(me, 2)
    x, y = lax.div(chip, side), lax.rem(chip, side)
    mine = (1 - core) * x + core * y, (1 - core) * y + core * x

    def place(net, at, dr, ds):
        r, s = lax.rem(at[0] + dr + side, side), lax.rem(at[1] + ds + side, side)
        xx, yy = (1 - net) * r + net * s, (1 - net) * s + net * r
        return (xx * side + yy) * 2

    def dev(dr, ds, other=False):
        return {"band": place(core, mine, dr, ds) + (1 - core if other else core)}

    def source(net, dr, ds):
        n = core * (1 - net) + (1 - core) * net
        return place(n, ((1 - n) * x + n * y, (1 - n) * y + n * x), dr, ds) + n

    partner = dev(0, 0, True)

    def send(src, dst, ssem, rsem, to):
        pltpu.make_async_remote_copy(
            src_ref=src, dst_ref=dst, send_sem=ssem, recv_sem=rsem, device_id=to, device_id_type=MESH
        ).start()

    def take(ref, sem):
        pltpu.make_async_remote_copy(
            src_ref=ref, dst_ref=ref, send_sem=sem, recv_sem=sem, device_id=partner, device_id_type=MESH
        ).wait_recv()

    def drain(ref, sem):
        pltpu.make_async_remote_copy(
            src_ref=ref, dst_ref=ref, send_sem=sem, recv_sem=sem, device_id=partner, device_id_type=MESH
        ).wait_send()

    barrier = pltpu.get_barrier_semaphore()
    greeted = [partner]
    for d in (-1, 1):
        for other in (False, True):
            greeted += [dev(d, 0, other), dev(0, d, other)]
    for to in greeted:
        pl.semaphore_signal(barrier, inc=1, device_id=to, device_id_type=MESH)

    n_band = table.shape[1]
    lane = lax.broadcasted_iota(jnp.int32, (1, n_band), 1)

    def fold(k, rows):
        rows = list(rows)
        for q in range(n_q):
            stored = home_ref[cand_ref[q, k]]
            who = lax.div(stored, own_ref.shape[0])
            hit = lane == who
            if q < 2:
                rows[0] = jnp.where(hit, stored - who * own_ref.shape[0], rows[0])
                rows[4] = jnp.where(hit, q, rows[4])
            rows[1 + q] = jnp.where(hit, valid_ref[q, k], rows[1 + q])
        return tuple(rows)

    for load in load_tables:
        load.wait()
    blank = jnp.zeros((1, n_band), jnp.int32)
    built = lax.fori_loop(0, cand_ref.shape[1], fold, (blank,) * 5, unroll=8)
    for r in range(5):
        table[pl.ds(r, 1), :] = built[r]
    pl.semaphore_wait(barrier, len(greeted))

    def head(j):
        return own_ref if j == 0 else spine.at[j - 1, 2]

    def spine_send(way, hop, t):
        src = own_ref.at[t] if hop == 1 else spine.at[way, hop - 2, t]
        send(src, spine.at[way, hop - 1, t], s_spine, r_spine.at[way, hop - 1, t], dev(0, 1 - 2 * way))

    def row_send(j, way, hop, t):
        src = head(j).at[t] if hop == 1 else row.at[j, ring_slot(way, hop - 1), t]
        dst = row.at[j, ring_slot(way, hop), t]
        sem = r_row.at[j, ring_slot(way, hop), t]
        if hop == 4:
            part = pl.ds(way * half, half)
            src, dst, sem = src.at[part], dst.at[part], r_row.at[j, 6 + way, t]
        send(src, dst, s_row.at[j], sem, dev(1 - 2 * way, 0))

    def row_take(j, way, hop, t):
        ref = row.at[j, ring_slot(way, hop), t]
        if hop == 4:
            take(ref.at[pl.ds(way * half, half)], r_row.at[j, 6 + way, t])
        else:
            take(ref, r_row.at[j, ring_slot(way, hop), t])

    load_own.wait()
    for t in range(3):
        for way in range(2):
            spine_send(way, 1, t)
            row_send(0, way, 1, t)

    send(table, tabv.at[0], s_tab, r_tab, dev(0, -1))
    send(table, tabv.at[1], s_tab, r_tab, dev(0, 1))
    send(table, tabv.at[2], s_tab, r_tab, dev(-1, 0, True))
    send(table, tabv.at[3], s_tab, r_tab, dev(1, 0, True))
    send(table, tabv.at[4], s_tab, r_tab, partner)
    own_tab = pltpu.make_async_copy(table, tabs.at[5], l_tab.at[0])
    own_tab.start()

    def init():
        load_q.wait()
        for q in range(n_q):
            scaled = q_ref[q].astype(jnp.float32).T * scale
            hi = scaled.astype(qt.dtype)
            qt[q, pl.ds(0, channels), :] = hi
            qt[q, pl.ds(channels, channels), :] = (scaled - hi.astype(jnp.float32)).astype(qt.dtype)
        acc[...] = jnp.zeros_like(acc)
        mx[...] = jnp.full_like(mx, NEG)

    def own():
        own_tab.wait()
        take(tabv, r_tab)
        got = pltpu.make_async_copy(tabv, tabs.at[pl.ds(0, 5)], l_tab.at[1])
        got.start()
        got.wait()
        pack_trunk(own_ref, me, kfg.at[0, 0], 0, kfg.at[1, 0], r_g.at[1], [])

    def pack(src, who, outs):
        step = 64
        for lo in range(0, rows_q, step):
            tiles = [src[t, pl.ds(lo, step), :] for t in range(3)]
            for table, dst, first, count in outs:
                if first <= lo < first + count:
                    which = tabs[table, 0, who]
                    dst[pl.ds(lo - first, step), :] = jnp.where(
                        which == 0, tiles[0], jnp.where(which == 1, tiles[1], tiles[2])
                    )

    up = (dev(0, 1), dev(0, 1, True))
    down = (dev(0, -1), dev(0, -1, True))
    whole = (0, rows_q)
    low, high = (0, half), (half, half)

    def pack_trunk(src, who, place_self, index_p, place_p, sem_p, more):
        outs = [(5, place_self, *whole), (4, st_p.at[index_p], *whole)]
        outs += [(table, stage, *rng) for table, stage, rng, *_ in more]
        pack(src, who, outs)
        for _, stage, _, dst, ssem, rsem, to in more:
            send(stage, dst, ssem, rsem, to)
        send(st_p.at[index_p], place_p, s_p, sem_p, partner)

    def pack_row(j, k):
        who = source(0, row_offset(k), HEAD[j])
        more = []
        for o in range(2):
            t_up, t_dn = 2 * o, 2 * o + 1
            if j == 0:
                more.append((t_up, st_a.at[k, o], whole, kfa.at[o, k, 1], s_a, r_a.at[o, k], up[o]))
                more.append((t_dn, st_a.at[k, 2 + o], whole, kfa.at[o, k, 2], s_a, r_a.at[o, k], down[o]))
            elif j == 1:
                more.append((t_dn, st_b1d.at[k, o], whole, kfb.at[o, k, 3], s_b1d, r_b.at[o, k], down[o]))
                more.append((t_up, st_b1u.at[k, o], low, kfb.at[o, k, 4, pl.ds(0, half)], s_b1u, r_b.at[o, k], up[o]))
            else:
                more.append((t_up, st_b2u.at[k, o], whole, kfb.at[o, k, 2], s_b2u, r_b.at[o, k], up[o]))
                more.append((t_dn, st_b2d.at[k, o], high, kfb.at[o, k, 4, pl.ds(half, half)], s_b2d, r_b.at[o, k], down[o]))
        if j == 0:
            pack_trunk(row.at[j, k], who, kfa.at[0, k, 0], 7 + k, kfa.at[1, k, 0], r_a.at[1, k], more)
        else:
            pack_trunk(row.at[j, k], who, kfb.at[0, k, j - 1], 7 + 7 * j + k, kfb.at[1, k, j - 1], r_b.at[1, k], more)

    def pack_spine(way, hop):
        slot = 2 * hop - 1 + way
        more = []
        if hop == 3:
            for o in range(2):
                if way == 0:
                    more.append((2 * o, st_b1u.at[7, o], low, kfg.at[o, 7, pl.ds(0, half)], s_b1u, r_g.at[2 * o], up[o]))
                else:
                    more.append((2 * o + 1, st_b2d.at[7, o], high, kfg.at[o, 7, pl.ds(half, half)], s_b2d, r_g.at[2 * o], down[o]))
        pack_trunk(spine.at[way, hop - 1], source(0, 0, LEAF_G[slot]), kfg.at[0, slot], slot, kfg.at[1, slot], r_g.at[1 if slot < NEAR else 2], more)

    scores, probs, tops = (sc0, sc1), (pr0, pr1), (tp0, tp1)
    ext = channels + 16

    def attend(units, width, ref_of, whos_of):
        keys = width * rows_q

        def score(v, ref, whos):
            for t in range(width):
                k = ref[t]
                rhs = qt[2] if v == 1 else qt[tabs[5, 4, whos[t]]]
                s = jnp.dot(jnp.concatenate([k, k], axis=1), rhs, preferred_element_type=jnp.float32)
                scores[v][pl.ds(t * rows_q, rows_q), :] = s
                tops[v][t] = jnp.max(s, axis=0, keepdims=True)

        def soften(v, t, shift):
            rows = pl.ds(t * rows_q, rows_q)
            probs[v][rows, :] = jnp.exp2(scores[v][rows, :] - shift).astype(jnp.bfloat16)

        def bias(q, who):
            return jnp.where(tabs[5, 1 + q, who] > 0, 0.0, NEG).astype(jnp.float32)

        def unit(u, _):
            ref, whos = ref_of(u), whos_of(u)
            later = jnp.minimum(u + 1, units - 1)
            second = [tabs[5, 4, who] == 1 for who in whos]
            b = [[bias(q, who) for who in whos] for q in range(3)]
            for t in range(width):
                kt = jnp.concatenate([ref[t].T, jnp.ones((16, rows_q), jnp.bfloat16)], axis=0)
                none = jnp.zeros_like(kt)
                cols = pl.ds(t * rows_q, rows_q)
                ktb[pl.ds(0, ext), cols] = jnp.where(second[t], none, kt)
                ktb[pl.ds(ext, ext), cols] = jnp.where(second[t], kt, none)
                ktb[pl.ds(2 * ext, ext), cols] = kt
            score(1, ref, whos)
            before = [mx[q] for q in range(3)]
            now = list(before)
            for t in range(width):
                for q in range(2):
                    now[q] = jnp.maximum(now[q], tops[0][t] + b[q][t])
            for t in range(width):
                base = jnp.where(second[t], now[1], now[0]) - jnp.maximum(b[0][t], b[1][t])
                soften(0, t, jnp.maximum(base, tops[0][t]))
            pv = jnp.dot(ktb[pl.ds(0, 2 * ext), pl.ds(0, keys)], probs[0][pl.ds(0, keys), :],
                         preferred_element_type=jnp.float32)
            for q in range(2):
                acc[q] = acc[q] * jnp.exp2(before[q] - now[q]) + pv[q * ext:(q + 1) * ext]
            score(0, ref_of(later), whos_of(later))
            for t in range(width):
                now[2] = jnp.maximum(now[2], tops[1][t] + b[2][t])
            for t in range(width):
                soften(1, t, jnp.maximum(now[2] - b[2][t], tops[1][t]))
            pv = jnp.dot(ktb[pl.ds(2 * ext, ext), pl.ds(0, keys)], probs[1][pl.ds(0, keys), :],
                         preferred_element_type=jnp.float32)
            acc[2] = acc[2] * jnp.exp2(before[2] - now[2]) + pv
            for q in range(3):
                mx[q] = now[q]
            return 0

        score(0, ref_of(0), whos_of(0))
        lax.fori_loop(0, units, unit, 0)

    def attend_near():
        take(kfg.at[1, pl.ds(0, NEAR)], r_g.at[1])
        attend(2, NEAR, lambda u: kfg.at[u, pl.ds(0, NEAR)], lambda u: [source(u, 0, o) for o in LEAF_G[:NEAR]])

    def attend_far():
        far = len(LEAF_G) - NEAR
        take(kfg.at[0, 7], r_g.at[0])
        take(kfg.at[1, pl.ds(NEAR, far)], r_g.at[2])
        attend(2, far, lambda u: kfg.at[u, pl.ds(NEAR, far)], lambda u: [source(u, 0, o) for o in LEAF_G[NEAR:]])

    def attend_row(hop, ref, sem, skip, offs):
        ways = 2 if hop < 4 else 1
        for way in range(ways):
            k = ring_slot(way, hop)
            take(ref.at[0, k, pl.ds(skip, ref.shape[2] - skip)], sem.at[0, k])
            take(ref.at[1, k], sem.at[1, k])

        def at(u):
            return lax.div(u, ways), lax.rem(u, ways)

        def unit_ref(u):
            net, way = at(u)
            return ref.at[net, 3 * way + hop - 1 if hop < 4 else 6]

        def whos(u):
            net, way = at(u)
            dr = hop * (2 * way - 1) if hop < 4 else 4
            return [source(net, dr, o) for o in offs]

        attend(2 * ways, len(offs), unit_ref, whos)

    def spine_step(hop):
        for t in range(3):
            for way in range(2):
                take(spine.at[way, hop - 1, t], r_spine.at[way, hop - 1, t])
                if hop < 3:
                    spine_send(way, hop + 1, t)
                else:
                    for w in range(2):
                        row_send(1 + way, w, 1, t)

    def row_step(j, hop):
        for t in range(3):
            for way in range(2):
                row_take(j, way, hop, t)
                if hop < 4:
                    row_send(j, way, hop + 1, t)

    for step in PLAN:
        kind, hop = step[0], step[-1]
        if step == "init":
            init()
        elif step == "own":
            own()
        elif step == "near":
            attend_near()
        elif step == "far":
            attend_far()
        elif kind == "s":
            spine_step(int(hop))
        elif kind == "r":
            row_step(int(step[1]), int(hop))
        elif kind == "z":
            for way in range(2):
                pack_spine(way, int(hop))
        elif kind == "p":
            for way in range(2 if hop < "4" else 1):
                pack_row(int(step[1]), ring_slot(way, int(hop)))
        elif kind == "a":
            attend_row(int(hop), kfa, r_a, 1, LEAF_A)
        else:
            attend_row(int(hop), kfb, r_b, 2, LEAF_B)

    for q in range(n_q):
        out_ref[q] = (acc[q, pl.ds(0, channels), :] / acc[q, pl.ds(channels, 1), :]).T.astype(out_ref.dtype)

    drain(spine, s_spine)
    for j in range(3):
        drain(row.at[j], s_row.at[j])
    drain(st_a, s_a)
    drain(st_b1u, s_b1u)
    drain(st_b1d, s_b1d)
    drain(st_b2u, s_b2u)
    drain(st_b2d, s_b2d)
    drain(st_p, s_p)
    drain(tabv, s_tab)


def body(side, query_tiles, target, tile_home, candidates, valid_mask):
    n_band = 2 * side * side
    tiles_dev, rows_q, channels = target.shape
    half = rows_q // 2

    def tile(*lead):
        return pltpu.VMEM((*lead, rows_q, channels), target.dtype)

    def halves(*lead):
        return pltpu.VMEM((*lead, half, channels), target.dtype)

    dma = pltpu.SemaphoreType.DMA
    n_q, widest = query_tiles.shape[0], len(LEAF_B)
    scratch = [
        *[pltpu.SMEM(a.shape, a.dtype) for a in (tile_home, candidates, valid_mask)],
        tile(n_q), tile(tiles_dev), tile(2, 3, 3), tile(3, 7, 3), tile(7, 4), halves(8, 2), tile(7, 2), tile(7, 2), halves(8, 2), tile(28),
        tile(2, 7, 3), tile(2, 7, 5), tile(2, 8),
        pltpu.VMEM((8, n_band), jnp.int32), pltpu.VMEM((5, 8, n_band), jnp.int32), pltpu.SMEM((6, 8, n_band), jnp.int32),
        pltpu.VMEM((n_q, 2 * channels, rows_q), target.dtype),
        pltpu.VMEM((n_q, channels + 16, rows_q), jnp.float32),
        pltpu.VMEM((n_q, 1, rows_q), jnp.float32),
        pltpu.VMEM((3 * (channels + 16), widest * rows_q), target.dtype),
        *[pltpu.VMEM((widest * rows_q, rows_q), jnp.float32)] * 2,
        *[pltpu.VMEM((widest * rows_q, rows_q), target.dtype)] * 2,
        *[pltpu.VMEM((widest, 1, rows_q), jnp.float32)] * 2,
        dma, dma((2, 3, 3)), dma((3,)), dma((3, 8, 3)), dma, dma, dma, dma, dma, dma,
        dma((2, 7)), dma((2, 7)), dma((3,)), dma, dma, dma((7,)),
    ]
    stored = pl.BlockSpec(memory_space=pltpu.HBM)
    return pl.pallas_call(
        functools.partial(kernel, side),
        out_shape=jax.ShapeDtypeStruct(query_tiles.shape, query_tiles.dtype),
        in_specs=[stored] * 5,
        out_specs=pl.BlockSpec(memory_space=pltpu.VMEM),
        scratch_shapes=scratch,
        compiler_params=pltpu.CompilerParams(
            collective_id=0, has_side_effects=True, vmem_limit_bytes=60 * 1024 * 1024
        ),
    )(tile_home, candidates, valid_mask, query_tiles, target)


def solution(mesh):
    side = math.isqrt(mesh.shape["band"] // 2)
    in_specs = (
        P(("pairs", "band"), None, None),
        P(("pairs", "band"), None, None),
        P("pairs"),
        P(("pairs", "band"), None),
        P(("pairs", "band"), None),
    )
    out_specs = P(("pairs", "band"), None, None)
    return jax.shard_map(
        functools.partial(body, side), mesh=mesh, in_specs=in_specs, out_specs=out_specs, check_vma=False
    )
```

```python
import functools
import math

import jax
import jax.numpy as jnp
from jax import lax
from jax.experimental import pallas as pl
from jax.experimental.pallas import tpu as pltpu
from jax.sharding import PartitionSpec as P

NEG = -1e30
MESH = pl.DeviceIdType.MESH
HEAD = (0, -3, 3)
LEAF_B = (-3, 3, 2, -2, 4)
LEAF_A = (0, -1, 1)
LEAF_G = (0, -1, 1, -2, 2, -3, 3, 4)
NEAR = 5
PLAN = (
    "s1", "init", "r01", "s2", "own", "z1", "s3", "z3", "r02", "z2", "r21", "r11", "p01", "r03", "p21",
    "near", "r22", "p11", "p22", "far", "r12", "p12", "p03", "a1", "p02", "b1", "r04", "r23", "p04", "p23",
    "r13", "p13", "b2", "a3", "r24", "r14", "a2", "p24", "p14", "a4", "b3", "b4",
)


def ring_slot(way, hop):
    return 3 * way + hop - 1 if hop <= 3 else 6


def row_offset(k):
    return -(k + 1) if k < 3 else (k - 2 if k < 6 else 4)


def kernel(side, home_any, cand_any, valid_any, q_any, own_any, out_ref, *scratch):
    (home_ref, cand_ref, valid_ref, q_ref, own_ref, spine, row, st_a, st_b1u, st_b1d, st_b2u, st_b2d, st_p, kfa, kfb, kfg, table, tabv, tabs, qt, acc,
     mx, ktb, sc0, sc1, pr0, pr1, tp0, tp1, s_spine, r_spine, s_row, r_row, s_a, s_b1u, s_b1d, s_b2u, s_b2d, s_p,
     r_a, r_b, r_g, s_tab, r_tab, l_tab) = scratch
    load_own = pltpu.make_async_copy(own_any, own_ref, l_tab.at[2])
    load_q = pltpu.make_async_copy(q_any, q_ref, l_tab.at[3])
    load_tables = [
        pltpu.make_async_copy(src, dst, l_tab.at[4 + i])
        for i, (src, dst) in enumerate(((home_any, home_ref), (cand_any, cand_ref), (valid_any, valid_ref)))
    ]
    for load in (*load_tables, load_own, load_q):
        load.start()
    n_q, rows_q, channels = q_ref.shape
    half = rows_q // 2
    scale = math.log2(math.e) / math.sqrt(channels)
    me = lax.axis_index("band")
    core = lax.rem(me, 2)
    chip = lax.div(me, 2)
    x, y = lax.div(chip, side), lax.rem(chip, side)
    mine = (1 - core) * x + core * y, (1 - core) * y + core * x

    def place(net, at, dr, ds):
        r, s = lax.rem(at[0] + dr + side, side), lax.rem(at[1] + ds + side, side)
        xx, yy = (1 - net) * r + net * s, (1 - net) * s + net * r
        return (xx * side + yy) * 2

    def dev(dr, ds, other=False):
        return {"band": place(core, mine, dr, ds) + (1 - core if other else core)}

    def source(net, dr, ds):
        n = core * (1 - net) + (1 - core) * net
        return place(n, ((1 - n) * x + n * y, (1 - n) * y + n * x), dr, ds) + n

    partner = dev(0, 0, True)

    def send(src, dst, ssem, rsem, to):
        pltpu.make_async_remote_copy(
            src_ref=src, dst_ref=dst, send_sem=ssem, recv_sem=rsem, device_id=to, device_id_type=MESH
        ).start()

    def take(ref, sem):
        pltpu.make_async_remote_copy(
            src_ref=ref, dst_ref=ref, send_sem=sem, recv_sem=sem, device_id=partner, device_id_type=MESH
        ).wait_recv()

    def drain(ref, sem):
        pltpu.make_async_remote_copy(
            src_ref=ref, dst_ref=ref, send_sem=sem, recv_sem=sem, device_id=partner, device_id_type=MESH
        ).wait_send()

    barrier = pltpu.get_barrier_semaphore()
    greeted = [partner]
    for d in (-1, 1):
        for other in (False, True):
            greeted += [dev(d, 0, other), dev(0, d, other)]
    for to in greeted:
        pl.semaphore_signal(barrier, inc=1, device_id=to, device_id_type=MESH)

    n_band = table.shape[1]
    lane = lax.broadcasted_iota(jnp.int32, (1, n_band), 1)

    def fold(k, rows):
        rows = list(rows)
        for q in range(n_q):
            stored = home_ref[cand_ref[q, k]]
            who = lax.div(stored, own_ref.shape[0])
            hit = lane == who
            if q < 2:
                rows[0] = jnp.where(hit, stored - who * own_ref.shape[0], rows[0])
                rows[4] = jnp.where(hit, q, rows[4])
            rows[1 + q] = jnp.where(hit, valid_ref[q, k], rows[1 + q])
        return tuple(rows)

    for load in load_tables:
        load.wait()
    blank = jnp.zeros((1, n_band), jnp.int32)
    built = lax.fori_loop(0, cand_ref.shape[1], fold, (blank,) * 5, unroll=8)
    for r in range(5):
        table[pl.ds(r, 1), :] = built[r]
    pl.semaphore_wait(barrier, len(greeted))

    def head(j):
        return own_ref if j == 0 else spine.at[j - 1, 2]

    def spine_send(way, hop, t):
        src = own_ref.at[t] if hop == 1 else spine.at[way, hop - 2, t]
        send(src, spine.at[way, hop - 1, t], s_spine, r_spine.at[way, hop - 1, t], dev(0, 1 - 2 * way))

    def row_send(j, way, hop, t):
        src = head(j).at[t] if hop == 1 else row.at[j, ring_slot(way, hop - 1), t]
        dst = row.at[j, ring_slot(way, hop), t]
        sem = r_row.at[j, ring_slot(way, hop), t]
        if hop == 4:
            part = pl.ds(way * half, half)
            src, dst, sem = src.at[part], dst.at[part], r_row.at[j, 6 + way, t]
        send(src, dst, s_row.at[j], sem, dev(1 - 2 * way, 0))

    def row_take(j, way, hop, t):
        ref = row.at[j, ring_slot(way, hop), t]
        if hop == 4:
            take(ref.at[pl.ds(way * half, half)], r_row.at[j, 6 + way, t])
        else:
            take(ref, r_row.at[j, ring_slot(way, hop), t])

    load_own.wait()
    for t in range(3):
        for way in range(2):
            spine_send(way, 1, t)
            row_send(0, way, 1, t)

    send(table, tabv.at[0], s_tab, r_tab, dev(0, -1))
    send(table, tabv.at[1], s_tab, r_tab, dev(0, 1))
    send(table, tabv.at[2], s_tab, r_tab, dev(-1, 0, True))
    send(table, tabv.at[3], s_tab, r_tab, dev(1, 0, True))
    send(table, tabv.at[4], s_tab, r_tab, partner)
    own_tab = pltpu.make_async_copy(table, tabs.at[5], l_tab.at[0])
    own_tab.start()

    def init():
        load_q.wait()
        for q in range(n_q):
            scaled = q_ref[q].astype(jnp.float32).T * scale
            hi = scaled.astype(qt.dtype)
            qt[q, pl.ds(0, channels), :] = hi
            qt[q, pl.ds(channels, channels), :] = (scaled - hi.astype(jnp.float32)).astype(qt.dtype)
        acc[...] = jnp.zeros_like(acc)
        mx[...] = jnp.full_like(mx, NEG)

    def own():
        own_tab.wait()
        take(tabv, r_tab)
        got = pltpu.make_async_copy(tabv, tabs.at[pl.ds(0, 5)], l_tab.at[1])
        got.start()
        got.wait()
        pack_trunk(own_ref, me, kfg.at[0, 0], 0, kfg.at[1, 0], r_g.at[1], [])

    def pack(src, who, outs):
        step = 64
        for lo in range(0, rows_q, step):
            tiles = [src[t, pl.ds(lo, step), :] for t in range(3)]
            for table, dst, first, count in outs:
                if first <= lo < first + count:
                    which = tabs[table, 0, who]
                    dst[pl.ds(lo - first, step), :] = jnp.where(
                        which == 0, tiles[0], jnp.where(which == 1, tiles[1], tiles[2])
                    )

    up = (dev(0, 1), dev(0, 1, True))
    down = (dev(0, -1), dev(0, -1, True))
    whole = (0, rows_q)
    low, high = (0, half), (half, half)

    def pack_trunk(src, who, place_self, index_p, place_p, sem_p, more):
        outs = [(5, place_self, *whole), (4, st_p.at[index_p], *whole)]
        outs += [(table, stage, *rng) for table, stage, rng, *_ in more]
        pack(src, who, outs)
        for _, stage, _, dst, ssem, rsem, to in more:
            send(stage, dst, ssem, rsem, to)
        send(st_p.at[index_p], place_p, s_p, sem_p, partner)

    def pack_row(j, k):
        who = source(0, row_offset(k), HEAD[j])
        more = []
        for o in range(2):
            t_up, t_dn = 2 * o, 2 * o + 1
            if j == 0:
                more.append((t_up, st_a.at[k, o], whole, kfa.at[o, k, 1], s_a, r_a.at[o, k], up[o]))
                more.append((t_dn, st_a.at[k, 2 + o], whole, kfa.at[o, k, 2], s_a, r_a.at[o, k], down[o]))
            elif j == 1:
                more.append((t_dn, st_b1d.at[k, o], whole, kfb.at[o, k, 3], s_b1d, r_b.at[o, k], down[o]))
                more.append((t_up, st_b1u.at[k, o], low, kfb.at[o, k, 4, pl.ds(0, half)], s_b1u, r_b.at[o, k], up[o]))
            else:
                more.append((t_up, st_b2u.at[k, o], whole, kfb.at[o, k, 2], s_b2u, r_b.at[o, k], up[o]))
                more.append((t_dn, st_b2d.at[k, o], high, kfb.at[o, k, 4, pl.ds(half, half)], s_b2d, r_b.at[o, k], down[o]))
        if j == 0:
            pack_trunk(row.at[j, k], who, kfa.at[0, k, 0], 7 + k, kfa.at[1, k, 0], r_a.at[1, k], more)
        else:
            pack_trunk(row.at[j, k], who, kfb.at[0, k, j - 1], 7 + 7 * j + k, kfb.at[1, k, j - 1], r_b.at[1, k], more)

    def pack_spine(way, hop):
        slot = 2 * hop - 1 + way
        more = []
        if hop == 3:
            for o in range(2):
                if way == 0:
                    more.append((2 * o, st_b1u.at[7, o], low, kfg.at[o, 7, pl.ds(0, half)], s_b1u, r_g.at[2 * o], up[o]))
                else:
                    more.append((2 * o + 1, st_b2d.at[7, o], high, kfg.at[o, 7, pl.ds(half, half)], s_b2d, r_g.at[2 * o], down[o]))
        pack_trunk(spine.at[way, hop - 1], source(0, 0, LEAF_G[slot]), kfg.at[0, slot], slot, kfg.at[1, slot], r_g.at[1 if slot < NEAR else 2], more)

    scores, probs, tops = (sc0, sc1), (pr0, pr1), (tp0, tp1)
    ext = channels + 16

    def attend(units, width, ref_of, whos_of):
        keys = width * rows_q

        def score(v, ref, whos):
            for t in range(width):
                k = ref[t]
                rhs = qt[2] if v == 1 else qt[tabs[5, 4, whos[t]]]
                s = jnp.dot(jnp.concatenate([k, k], axis=1), rhs, preferred_element_type=jnp.float32)
                scores[v][pl.ds(t * rows_q, rows_q), :] = s
                tops[v][t] = jnp.max(s, axis=0, keepdims=True)

        def soften(v, t, shift):
            rows = pl.ds(t * rows_q, rows_q)
            probs[v][rows, :] = jnp.exp2(scores[v][rows, :] - shift).astype(jnp.bfloat16)

        def bias(q, who):
            return jnp.where(tabs[5, 1 + q, who] > 0, 0.0, NEG).astype(jnp.float32)

        def unit(u, _):
            ref, whos = ref_of(u), whos_of(u)
            later = jnp.minimum(u + 1, units - 1)
            second = [tabs[5, 4, who] == 1 for who in whos]
            b = [[bias(q, who) for who in whos] for q in range(3)]
            for t in range(width):
                kt = jnp.concatenate([ref[t].T, jnp.ones((16, rows_q), jnp.bfloat16)], axis=0)
                none = jnp.zeros_like(kt)
                cols = pl.ds(t * rows_q, rows_q)
                ktb[pl.ds(0, ext), cols] = jnp.where(second[t], none, kt)
                ktb[pl.ds(ext, ext), cols] = jnp.where(second[t], kt, none)
                ktb[pl.ds(2 * ext, ext), cols] = kt
            score(1, ref, whos)
            before = [mx[q] for q in range(3)]
            now = list(before)
            for t in range(width):
                for q in range(2):
                    now[q] = jnp.maximum(now[q], tops[0][t] + b[q][t])
            for t in range(width):
                base = jnp.where(second[t], now[1], now[0]) - jnp.maximum(b[0][t], b[1][t])
                soften(0, t, jnp.maximum(base, tops[0][t]))
            for q in range(2):
                pv = jnp.dot(ktb[pl.ds(q * ext, ext), pl.ds(0, keys)], probs[0][pl.ds(0, keys), :],
                             preferred_element_type=jnp.float32)
                acc[q] = acc[q] * jnp.exp2(before[q] - now[q]) + pv
            score(0, ref_of(later), whos_of(later))
            for t in range(width):
                now[2] = jnp.maximum(now[2], tops[1][t] + b[2][t])
            for t in range(width):
                soften(1, t, jnp.maximum(now[2] - b[2][t], tops[1][t]))
            pv = jnp.dot(ktb[pl.ds(2 * ext, ext), pl.ds(0, keys)], probs[1][pl.ds(0, keys), :],
                         preferred_element_type=jnp.float32)
            acc[2] = acc[2] * jnp.exp2(before[2] - now[2]) + pv
            for q in range(3):
                mx[q] = now[q]
            return 0

        score(0, ref_of(0), whos_of(0))
        lax.fori_loop(0, units, unit, 0)

    def attend_near():
        take(kfg.at[1, pl.ds(0, NEAR)], r_g.at[1])
        attend(2, NEAR, lambda u: kfg.at[u, pl.ds(0, NEAR)], lambda u: [source(u, 0, o) for o in LEAF_G[:NEAR]])

    def attend_far():
        far = len(LEAF_G) - NEAR
        take(kfg.at[0, 7], r_g.at[0])
        take(kfg.at[1, pl.ds(NEAR, far)], r_g.at[2])
        attend(2, far, lambda u: kfg.at[u, pl.ds(NEAR, far)], lambda u: [source(u, 0, o) for o in LEAF_G[NEAR:]])

    def attend_row(hop, ref, sem, skip, offs):
        ways = 2 if hop < 4 else 1
        for way in range(ways):
            k = ring_slot(way, hop)
            take(ref.at[0, k, pl.ds(skip, ref.shape[2] - skip)], sem.at[0, k])
            take(ref.at[1, k], sem.at[1, k])

        def at(u):
            return lax.div(u, ways), lax.rem(u, ways)

        def unit_ref(u):
            net, way = at(u)
            return ref.at[net, 3 * way + hop - 1 if hop < 4 else 6]

        def whos(u):
            net, way = at(u)
            dr = hop * (2 * way - 1) if hop < 4 else 4
            return [source(net, dr, o) for o in offs]

        attend(2 * ways, len(offs), unit_ref, whos)

    def spine_step(hop):
        for t in range(3):
            for way in range(2):
                take(spine.at[way, hop - 1, t], r_spine.at[way, hop - 1, t])
                if hop < 3:
                    spine_send(way, hop + 1, t)
                else:
                    for w in range(2):
                        row_send(1 + way, w, 1, t)

    def row_step(j, hop):
        for t in range(3):
            for way in range(2):
                row_take(j, way, hop, t)
                if hop < 4:
                    row_send(j, way, hop + 1, t)

    for step in PLAN:
        kind, hop = step[0], step[-1]
        if step == "init":
            init()
        elif step == "own":
            own()
        elif step == "near":
            attend_near()
        elif step == "far":
            attend_far()
        elif kind == "s":
            spine_step(int(hop))
        elif kind == "r":
            row_step(int(step[1]), int(hop))
        elif kind == "z":
            for way in range(2):
                pack_spine(way, int(hop))
        elif kind == "p":
            for way in range(2 if hop < "4" else 1):
                pack_row(int(step[1]), ring_slot(way, int(hop)))
        elif kind == "a":
            attend_row(int(hop), kfa, r_a, 1, LEAF_A)
        else:
            attend_row(int(hop), kfb, r_b, 2, LEAF_B)

    for q in range(n_q):
        out_ref[q] = (acc[q, pl.ds(0, channels), :] / acc[q, pl.ds(channels, 1), :]).T.astype(out_ref.dtype)

    drain(spine, s_spine)
    for j in range(3):
        drain(row.at[j], s_row.at[j])
    drain(st_a, s_a)
    drain(st_b1u, s_b1u)
    drain(st_b1d, s_b1d)
    drain(st_b2u, s_b2u)
    drain(st_b2d, s_b2d)
    drain(st_p, s_p)
    drain(tabv, s_tab)


def body(side, query_tiles, target, tile_home, candidates, valid_mask):
    n_band = 2 * side * side
    tiles_dev, rows_q, channels = target.shape
    half = rows_q // 2

    def tile(*lead):
        return pltpu.VMEM((*lead, rows_q, channels), target.dtype)

    def halves(*lead):
        return pltpu.VMEM((*lead, half, channels), target.dtype)

    dma = pltpu.SemaphoreType.DMA
    n_q, widest = query_tiles.shape[0], len(LEAF_B)
    scratch = [
        *[pltpu.SMEM(a.shape, a.dtype) for a in (tile_home, candidates, valid_mask)],
        tile(n_q), tile(tiles_dev), tile(2, 3, 3), tile(3, 7, 3), tile(7, 4), halves(8, 2), tile(7, 2), tile(7, 2), halves(8, 2), tile(28),
        tile(2, 7, 3), tile(2, 7, 5), tile(2, 8),
        pltpu.VMEM((8, n_band), jnp.int32), pltpu.VMEM((5, 8, n_band), jnp.int32), pltpu.SMEM((6, 8, n_band), jnp.int32),
        pltpu.VMEM((n_q, 2 * channels, rows_q), target.dtype),
        pltpu.VMEM((n_q, channels + 16, rows_q), jnp.float32),
        pltpu.VMEM((n_q, 1, rows_q), jnp.float32),
        pltpu.VMEM((3 * (channels + 16), widest * rows_q), target.dtype),
        *[pltpu.VMEM((widest * rows_q, rows_q), jnp.float32)] * 2,
        *[pltpu.VMEM((widest * rows_q, rows_q), target.dtype)] * 2,
        *[pltpu.VMEM((widest, 1, rows_q), jnp.float32)] * 2,
        dma, dma((2, 3, 3)), dma((3,)), dma((3, 8, 3)), dma, dma, dma, dma, dma, dma,
        dma((2, 7)), dma((2, 7)), dma((3,)), dma, dma, dma((7,)),
    ]
    stored = pl.BlockSpec(memory_space=pltpu.HBM)
    return pl.pallas_call(
        functools.partial(kernel, side),
        out_shape=jax.ShapeDtypeStruct(query_tiles.shape, query_tiles.dtype),
        in_specs=[stored] * 5,
        out_specs=pl.BlockSpec(memory_space=pltpu.VMEM),
        scratch_shapes=scratch,
        compiler_params=pltpu.CompilerParams(
            collective_id=0, has_side_effects=True, vmem_limit_bytes=60 * 1024 * 1024
        ),
    )(tile_home, candidates, valid_mask, query_tiles, target)


def solution(mesh):
    side = math.isqrt(mesh.shape["band"] // 2)
    in_specs = (
        P(("pairs", "band"), None, None),
        P(("pairs", "band"), None, None),
        P("pairs"),
        P(("pairs", "band"), None),
        P(("pairs", "band"), None),
    )
    out_specs = P(("pairs", "band"), None, None)
    return jax.shard_map(
        functools.partial(body, side), mesh=mesh, in_specs=in_specs, out_specs=out_specs, check_vma=False
    )
```
